32 devices in a mesh: row: 8 (over z, core), col: 2 (over x), gz: 2 (over y).
Axes of the slice: x: 2, y: 2, z: 4, core: 2. Of those that a mesh axis runs over, the one named last changes fastest.
Arguments:
- initial_field: float32 [8, 32, 32, 256], P(None, 'row', 'col', 'gz'), may hold values from -6 to 6
- source_term: float32 [8, 32, 32, 256], P(None, 'row', 'col', 'gz'), may hold values from -6 to 6
- cell_class: int32 [32, 32, 256], P('row', 'col', 'gz'), may hold values from 0 to 15
- class_shift: float32 [16], replicated, may hold values from 0.05 to 4
- surface_cell: int32 [4096], P(('row', 'col', 'gz')), may hold values from 0 to 8191
- live_count: int32 [32], P(('row', 'col', 'gz')), may hold values from 1 to 128, 2560 in all
- panel_geometry: float32 [4, 4096], P(None, ('row', 'col', 'gz')), may hold values from 0.5 to 2
Outputs:
- final_field: float32 [8, 32, 32, 256], P(None, 'row', 'col', 'gz')
- boundary_potential: float32 [8, 4096], P(None, ('row', 'col', 'gz'))
The draws below stay inside these ranges and needn't reach their ends.
Inputs may be any that keep to these rules, and one draw needn't show every extreme that they name: Slots 0 to live_count[b] - 1 of brick b are in use; the counts sum to 2560. `surface_cell`: A cell index inside the panel's own brick, x * 16 * 128 + y * 128 + z.
All inputs are finite; a program needn't handle non-finite values. No bound on the sum of `live_count` on one device may be relied on, other than what follows from the above.
Results may differ from the reference program's by a relative error of at most 0.004.
Values may be sent and summed in bfloat16 or wider, within the bound.
A program may use at most 128 MiB of HBM per device.

```python
import math
import jax
import jax.numpy as jnp
import numpy as np
from jax import lax

EXC = 8
CLASSES = 16
CX = 4
CY = 16
CZ = 128
SLOTS = 128
SWEEPS = 3
ROUNDS = 2
NX = 32
NY = 32
NZ = 256
PANELS = 4096
N_COL = 2
N_GZ = 2
DEVICES = 32


def plant(result, stream_key, smallest, largest):
    index_at = [jax.random.randint(jax.random.fold_in(stream_key, axis), (), 0, length) for axis, length in enumerate(result.shape)]
    widest = result.shape.index(max(result.shape))
    beside = index_at[:widest] + [(index_at[widest] + 1) % result.shape[widest]] + index_at[widest + 1:]
    return result.at[tuple(index_at)].set(smallest).at[tuple(beside)].set(largest)


def shard_levels(key, extent, pieces, smallest, high):
    loudness = 1.0
    for position, blocks in pieces:
        heights = jax.random.uniform(jax.random.fold_in(jax.random.fold_in(key, 6), position), (blocks,), jnp.float32, smallest / len(pieces), high / len(pieces))
        loudness = loudness * jnp.repeat(jnp.exp(heights), extent[position] // blocks).reshape((-1,) + (1,) * (len(extent) - 1 - position))
    return loudness


def split_up(count, total, most, lean):
    weights = [(1 << 20) // math.isqrt(grade ** lean) + 1 for grade in range(2, count + 1)]
    spare, holding = total - most - (count - 1), [1] * (count - 1)
    while spare > 0:
        candidates = [i for i in range(count - 1) if holding[i] < most]
        mass, budget = sum([weights[i] for i in candidates]), spare
        for i in candidates:
            extra = min(most - holding[i], max(1, budget * weights[i] // mass), spare)
            holding[i] = holding[i] + extra
            spare = spare - extra
    return np.array([most] + holding)


def uneven_parts(own_key, number_of, total, limit, slope):
    if number_of == 2:
        one = jax.random.randint(own_key, (), max(1, total - limit), min(limit, total - 1) + 1)
        return jnp.stack([one, total - one])
    tallies = jnp.asarray(split_up(number_of, total, limit, slope), jnp.int32)
    couples = (number_of - 1) // 2
    donor, receiver = tallies[1:1 + 2 * couples:2], tallies[2:2 + 2 * couples:2]
    room = jnp.minimum(donor - 1, limit - receiver)
    shifted = jax.random.randint(jax.random.fold_in(own_key, 1), (couples,), 0, 1 << 20) % (room + 1)
    tallies = tallies.at[1:1 + 2 * couples:2].set(donor - shifted).at[2:2 + 2 * couples:2].set(receiver + shifted)
    return tallies[jax.random.permutation(jax.random.fold_in(own_key, 2), number_of)]


def bell_draw(stream_key, extent, scale, most, cuts=(), held_as=jnp.bfloat16):
    values = jax.random.normal(stream_key, extent, jnp.float32) * scale
    if len(cuts) > 0:
        values = shard_levels(stream_key, extent, cuts, -0.22, 0.18) * values
    return jnp.clip(values, min=-most, max=most).astype(held_as)


def setup_inputs(seed: int = 0) -> dict:
    seeds = jax.random.split(jax.random.key(seed), 8)
    return {
        "initial_field": bell_draw(seeds[0], (EXC, NX, NY, NZ), 1.0, 6.0, ((1, 8), (2, 2), (3, 2)), jnp.float32),
        "source_term": bell_draw(seeds[1], (EXC, NX, NY, NZ), 1.0, 6.0, ((1, 8), (2, 2), (3, 2)), jnp.float32),
        "cell_class": plant(jax.random.randint(seeds[2], (NX, NY, NZ), 0, CLASSES), jax.random.fold_in(seeds[2], 1), 0, CLASSES - 1).astype(jnp.int32),
        "class_shift": jnp.clip(jnp.exp(jax.random.uniform(seeds[3], (CLASSES,), jnp.float32, math.log(0.05), math.log(4.0))), 0.05, 4.0),
        "surface_cell": plant(jax.random.randint(seeds[4], (PANELS,), 0, CX * CY * CZ), jax.random.fold_in(seeds[4], 1), 0, (CX * CY * CZ) - 1).astype(jnp.int32),
        "live_count": uneven_parts(seeds[5], DEVICES, PANELS * 5 // 8, SLOTS, 2).astype(jnp.int32),
        "panel_geometry": jnp.clip(0.5 + 1.5 * jax.random.uniform(seeds[6], (4, PANELS), jnp.float32) ** shard_levels(seeds[6], (4, PANELS), ((1, 32),), -0.2, 0.2), 0.5, 2.0),
    }


relax_weight = 0.8
wave_number = 25.0
soften = 0.05
coupling = 0.5

def neighbours(padded):
    total = padded[:, 2:, 1:-1, 1:-1] + padded[:, :-2, 1:-1, 1:-1]
    total = total + padded[:, 1:-1, 2:, 1:-1] + padded[:, 1:-1, :-2, 1:-1]
    total = total + padded[:, 1:-1, 1:-1, 2:] + padded[:, 1:-1, 1:-1, :-2]
    return total

def relax(state, padded, forcing, shift_field):
    diagonal = 6.0 + shift_field
    residual = forcing - (diagonal * state - neighbours(padded))
    return state + relax_weight * residual / diagonal

def kernel_tile(sources, targets, factor):
    delta_x = targets[0][None, :] - sources[0][:, None]
    delta_y = targets[1][None, :] - sources[1][:, None]
    delta_z = targets[2][None, :] - sources[2][:, None]
    distance = jnp.sqrt(delta_x * delta_x + delta_y * delta_y + delta_z * delta_z)
    values = sources[3][:, None] * jnp.cos(wave_number * distance) / (distance + soften)
    return (values * factor).astype(jnp.bfloat16)

def reference(initial_field, source_term, cell_class, class_shift, surface_cell, live_count, panel_geometry):
    shift_field = class_shift[cell_class]
    factor = 1.0 / math.sqrt(PANELS)
    slot_index = jnp.arange(PANELS, dtype=jnp.int32)
    owner = (slot_index // SLOTS).astype(jnp.int32)
    live = (slot_index % SLOTS < live_count[owner]).astype(jnp.float32)
    brick_row = owner // (N_COL * N_GZ)
    brick_col = owner // N_GZ % N_COL
    brick_depth = owner % N_GZ
    global_x = brick_row * CX + surface_cell // (CY * CZ)
    global_y = brick_col * CY + surface_cell // CZ % CY
    global_z = brick_depth * CZ + surface_cell % CZ
    cell_of = ((global_x * NY + global_y) * NZ + global_z).astype(jnp.int32)
    width = math.gcd(PANELS, 512)
    blocks = panel_geometry.reshape(4, PANELS // width, width).transpose(1, 0, 2)
    state = initial_field
    load = jnp.zeros_like(source_term)
    potential = jnp.zeros((EXC, PANELS), jnp.float32)
    for round_index in range(ROUNDS):
        forcing = source_term + load
        for sweep_index in range(SWEEPS):
            padded = jnp.pad(state, ((0, 0), (1, 1), (1, 1), (1, 1)))
            state = relax(state, padded, forcing, shift_field)
        density = (state.reshape(EXC, -1)[:, cell_of] * live).astype(jnp.bfloat16)
        density = lax.optimization_barrier(density).astype(jnp.float32)

        def target_block(targets):
            tile = lax.optimization_barrier(kernel_tile(panel_geometry, targets, factor)).astype(jnp.float32)
            return jnp.dot(density, tile, precision=lax.Precision.HIGHEST)
        potential = lax.map(target_block, blocks)
        potential = potential.transpose(1, 0, 2).reshape(EXC, PANELS) * live
        if round_index + 1 < ROUNDS:
            spread = jnp.zeros((EXC, NX * NY * NZ), jnp.float32).at[:, cell_of].add(coupling * potential)
            load = spread.reshape(source_term.shape)
    return (state, potential)
```

```python
import functools
import math

import jax
import jax.numpy as jnp
import numpy as np
from jax import lax
from jax.experimental import pallas as pl
from jax.experimental.pallas import tpu as pltpu
from jax.sharding import PartitionSpec as P

SWEEPS = 3
ROUNDS = 2
STEPS = SWEEPS * ROUNDS

relax_weight = 0.8
wave_number = 25.0
soften = 0.05
coupling = 0.5

MESH = pl.DeviceIdType.MESH
AXES = ("row", "col", "gz")


def cosine_terms(degree=8):
    nodes = 0.125 * (1.0 + np.cos(np.pi * (np.arange(64) + 0.5) / 64))
    fitted = np.polynomial.Polynomial.fit(
        nodes, np.cos(2 * np.pi * np.sqrt(nodes)), degree, domain=[0.0, 0.25]
    )
    return [float(c) for c in fitted.convert().coef]


COSINE = cosine_terms()


def cosine_of_turns(turns):
    fraction = turns - jnp.floor(turns + 0.5)
    square = fraction * fraction
    value = jnp.full_like(square, COSINE[-1])
    for term in reversed(COSINE[:-1]):
        value = value * square + term
    return value


def kernel(
    sizes,
    init_hbm, source_hbm, class_hbm, shift_ref, cell_ref, live_ref, geo_ref,
    field_ref, potential_ref,
    init_v, source_v, class_v, weight_v, state_v, forcing_v,
    x_out, x_in, y_out, y_in, z_out, z_in,
    geo_all, column_v, tile_v, density_out, density_all,
    local_sem, face_send, face_recv, geo_sem, density_sem,
):
    rows, cols, depths = sizes
    devices = rows * cols * depths
    channels, size_x, size_y, size_z = init_hbm.shape
    slots = cell_ref.shape[1]
    classes = shift_ref.shape[0]
    factor = 1.0 / math.sqrt(slots * devices)
    here = tuple(lax.axis_index(axis) for axis in AXES)
    me = (here[0] * cols + here[1]) * depths + here[2]

    copies = [
        pltpu.make_async_copy(init_hbm, init_v, local_sem.at[0]),
        pltpu.make_async_copy(class_hbm, class_v, local_sem.at[1]),
        pltpu.make_async_copy(source_hbm, source_v, local_sem.at[2]),
    ]
    for copy in copies:
        copy.start()

    def each_other(action):
        def at(a, first):
            row = lax.rem(here[0] + a, rows)
            for b in range(cols):
                for c in range(depths):
                    if first and b == 0 and c == 0:
                        continue
                    action((row, lax.rem(here[1] + b, cols), lax.rem(here[2] + c, depths)))

        def others(i, carry):
            at(i, False)
            return carry

        lax.fori_loop(1, rows, others, 0)
        at(0, True)

    barrier = pltpu.get_barrier_semaphore()
    each_other(
        lambda device: pl.semaphore_signal(barrier, inc=1, device_id=device, device_id_type=MESH)
    )

    lane = lax.broadcasted_iota(jnp.int32, (size_y, size_z), 1)
    line = lax.broadcasted_iota(jnp.int32, (size_y, size_z), 0)
    half = size_z // 2

    def pack(k, e, x, value, packed):
        if x == 0:
            x_out[k, 0, e] = value.astype(x_out.dtype)
        if x == size_x - 1:
            x_out[k, 1, e] = value.astype(x_out.dtype)
        y_out[k, 0, e, x : x + 1, :] = value[0:1, :]
        y_out[k, 1, e, x : x + 1, :] = value[size_y - 1 : size_y, :]
        at = e * size_x + x
        low = jnp.broadcast_to(value[:, 0:1], value.shape)
        high = jnp.broadcast_to(value[:, size_z - 1 : size_z], value.shape)
        packed = jnp.where(lane == at, low, packed)
        return jnp.where(lane == at + half, high, packed)

    def face_copies(k):
        made = []
        for axis, (send, receive) in enumerate(((x_out, x_in), (y_out, y_in), (z_out, z_in))):
            count = sizes[axis]
            if count == 1:
                continue
            for up in (0, 1):
                target = {AXES[axis]: here[axis] + (1 if up else -1)}
                source = send.at[k] if axis == 2 else send.at[k, up]
                copy = pltpu.make_async_remote_copy(
                    src_ref=source,
                    dst_ref=receive.at[k, 1 - up],
                    send_sem=face_send.at[k, 2 * axis + up],
                    recv_sem=face_recv.at[k, 2 * axis + 1 - up],
                    device_id=target,
                    device_id_type=MESH,
                )
                sends = here[axis] < count - 1 if up else here[axis] > 0
                gets = here[axis] > 0 if up else here[axis] < count - 1
                made.append((copy, sends, gets))
        return made

    def start_faces(k):
        for copy, sends, _ in face_copies(k):
            pl.when(sends)(copy.start)

    def await_faces(k):
        for copy, _, gets in face_copies(k):
            pl.when(gets)(copy.wait_recv)

    def finish_faces(k):
        for copy, sends, _ in face_copies(k):
            pl.when(sends)(copy.wait_send)

    x_in[STEPS] = jnp.zeros(x_in.shape[1:], x_in.dtype)
    y_in[STEPS] = jnp.zeros(y_in.shape[1:], y_in.dtype)
    z_in[STEPS] = jnp.zeros(z_in.shape[1:], z_in.dtype)

    copies[0].wait()

    def pack_first(e, packed):
        for x in range(size_x):
            packed = pack(0, e, x, init_v[e, x], packed)
        return packed

    z_out[0] = lax.fori_loop(
        0, channels, pack_first, jnp.zeros((size_y, size_z), jnp.float32), unroll=True
    )

    eye = lax.broadcasted_iota(jnp.int32, (slots, slots), 0) == lax.broadcasted_iota(
        jnp.int32, (slots, slots), 1
    )
    for i in range(3):
        column = jnp.sum(jnp.where(eye, geo_ref[i : i + 1, :], 0.0), axis=1, keepdims=True)
        column_v[i] = jnp.broadcast_to(column, (slots, slots))
    geo_all[me] = geo_ref[...]

    pl.semaphore_wait(barrier, devices - 1)
    start_faces(0)

    def gather_copy(source, gathered, sems, device):
        return pltpu.make_async_remote_copy(
            src_ref=source,
            dst_ref=gathered.at[me],
            send_sem=sems.at[0],
            recv_sem=sems.at[1],
            device_id=device,
            device_id_type=MESH,
        )

    def start_gather(source, gathered, sems):
        each_other(lambda device: gather_copy(source, gathered, sems, device).start())

    def await_gather(gathered, sems, which):
        whole = gathered.at[pl.ds(0, devices - 1)]
        pltpu.make_async_copy(whole, whole, sems.at[which]).wait()

    start_gather(geo_ref, geo_all, geo_sem)

    copies[1].wait()
    for x in range(size_x):
        kind = class_v[x]
        shift = jnp.zeros(kind.shape, jnp.float32)
        for level in range(classes):
            shift = jnp.where(kind == level, shift_ref[level], shift)
        weight_v[x] = relax_weight / (6.0 + shift)

    cell = cell_ref[...]
    bits = size_z.bit_length() - 1
    cell_z = cell & (size_z - 1)
    cell_xy = cell >> bits
    pick_z = lax.broadcasted_iota(jnp.int32, (size_z, slots), 0) == cell_z
    pick_z = jnp.where(pick_z, 1.0, 0.0).astype(jnp.bfloat16)
    pick_xy = lax.broadcasted_iota(jnp.int32, (size_x * size_y, slots), 0) == cell_xy
    live = lax.broadcasted_iota(jnp.int32, (channels, slots), 1) < live_ref[0]
    which = lax.broadcasted_iota(jnp.int32, (channels, slots), 0)
    copies[2].wait()

    def sweep(k):
        now = (lambda e, x: init_v[e, x]) if k == 0 else (lambda e, x: state_v[k - 1, e, x])
        last = k == STEPS - 1
        force = source_v if k < SWEEPS else forcing_v
        slot = []
        for axis in range(3):
            below = jnp.where(here[axis] > 0, k, STEPS)
            above = jnp.where(here[axis] < sizes[axis] - 1, k, STEPS)
            slot.append((below, above))
        z_low, z_high = z_in[slot[2][0], 0], z_in[slot[2][1], 1]

        def body(e, packed):
            tiles = [now(e, x) for x in range(size_x)]
            before = x_in[slot[0][0], 0, e].astype(jnp.float32)
            after = x_in[slot[0][1], 1, e].astype(jnp.float32)
            spread = [before] + tiles + [after]
            for x in range(size_x):
                value = tiles[x]
                around = spread[x + 2] + spread[x]
                low = y_in[slot[1][0], 0, e, x : x + 1, :]
                high = y_in[slot[1][1], 1, e, x : x + 1, :]
                around = around + jnp.where(
                    line == size_y - 1, high, pltpu.roll(value, size_y - 1, 0)
                )
                around = around + jnp.where(line == 0, low, pltpu.roll(value, 1, 0))
                at = e * size_x + x
                high = pltpu.roll(z_high, lax.rem(2 * size_z - 1 - at, size_z), 1)
                low = pltpu.roll(z_low, lax.rem(size_z + half - at, size_z), 1)
                around = around + jnp.where(
                    lane == size_z - 1, high, pltpu.roll(value, size_z - 1, 1)
                )
                around = around + jnp.where(lane == 0, low, pltpu.roll(value, 1, 1))
                result = (1.0 - relax_weight) * value + weight_v[x] * (force[e, x] + around)
                if last:
                    field_ref[e, x] = result
                else:
                    state_v[k, e, x] = result
                    packed = pack(k + 1, e, x, result, packed)
            return packed

        packed = lax.fori_loop(
            0, channels, body, jnp.zeros((size_y, size_z), jnp.float32), unroll=2
        )
        if not last:
            z_out[k + 1] = packed

    pieces = 4
    chunk = slots // pieces

    def make_tiles(first, stop):
        def body(s, carry):
            source = geo_all[s]
            for piece in range(pieces):
                span = slice(piece * chunk, (piece + 1) * chunk)
                delta_x = column_v[0, span, :] - source[0:1, :]
                delta_y = column_v[1, span, :] - source[1:2, :]
                delta_z = column_v[2, span, :] - source[2:3, :]
                distance = jnp.sqrt(delta_x * delta_x + delta_y * delta_y + delta_z * delta_z)
                wave = cosine_of_turns(distance * (wave_number / (2.0 * math.pi)))
                value = (source[3:4, :] * factor) * wave / (distance + soften)
                tile_v[s, span, :] = value.astype(tile_v.dtype)
            return carry

        lax.fori_loop(first, stop, body, 0)

    group = math.gcd(devices, 8)

    def apply_tiles(gathered):
        def body(i, total):
            for j in range(group):
                s = i * group + j
                total = total + lax.dot_general(
                    gathered[s], tile_v[s], (((1,), (1,)), ((), ())),
                    preferred_element_type=jnp.float32,
                )
            return total

        return lax.fori_loop(
            0, devices // group, body, jnp.zeros((channels, slots), jnp.float32)
        )

    cut = [0, 3 * devices // 8, 3 * devices // 4, devices]
    for k in range(STEPS):
        if k == 1:
            await_gather(geo_all, geo_sem, 1)
        if k in (1, 2):
            make_tiles(cut[k - 1], cut[k])
        await_faces(k)
        sweep(k)
        end = k % SWEEPS == SWEEPS - 1
        if k + 1 < STEPS:
            start_faces(k + 1)
        if not end:
            continue
        r = k // SWEEPS
        ending = field_ref if k == STEPS - 1 else state_v.at[k]
        flat = ending[...].reshape(channels * size_x * size_y, size_z).astype(jnp.bfloat16)
        picked = jnp.dot(flat, pick_z, preferred_element_type=jnp.float32)
        density = jnp.zeros((channels, slots), jnp.float32)
        for e in range(channels):
            block = picked[e * size_x * size_y : (e + 1) * size_x * size_y]
            found = jnp.sum(jnp.where(pick_xy, block, 0.0), axis=0, keepdims=True)
            density = jnp.where(which == e, found, density)
        density = jnp.where(live, density, 0.0).astype(jnp.bfloat16)
        density_out[r] = density
        density_all[r, me] = density
        start_gather(density_out.at[r], density_all.at[r], density_sem.at[r])
        if r == 0:
            make_tiles(cut[2], cut[3])
        await_gather(density_all.at[r], density_sem.at[r], 1)
        potential = jnp.where(live, apply_tiles(density_all.at[r]), 0.0)
        if r == ROUNDS - 1:
            potential_ref[...] = potential
        else:
            half_of = coupling * potential
            big = half_of.astype(jnp.bfloat16).astype(jnp.float32)
            small = half_of - big
            for e in range(channels):
                load = jnp.zeros((size_x * size_y, size_z), jnp.float32)
                for part in (big, small):
                    placed = jnp.where(pick_xy, part[e : e + 1, :], 0.0).astype(jnp.bfloat16)
                    load = load + lax.dot_general(
                        placed, pick_z, (((1,), (1,)), ((), ())),
                        preferred_element_type=jnp.float32,
                    )
                forcing_v[e] = source_v[e] + load.reshape(size_x, size_y, size_z)

    for k in range(STEPS):
        finish_faces(k)
    await_gather(geo_all, geo_sem, 0)
    for r in range(ROUNDS):
        await_gather(density_all.at[r], density_sem.at[r], 0)


def local(sizes, initial_field, source_term, cell_class, class_shift, surface_cell, live_count,
          panel_geometry):
    channels, size_x, size_y, size_z = initial_field.shape
    slots = surface_cell.shape[0]
    devices = sizes[0] * sizes[1] * sizes[2]
    brick = (channels, size_x, size_y, size_z)
    vmem = pl.BlockSpec(memory_space=pltpu.VMEM)
    smem = pl.BlockSpec(memory_space=pltpu.SMEM)
    hbm = pl.BlockSpec(memory_space=pl.ANY)
    return pl.pallas_call(
        functools.partial(kernel, sizes),
        out_shape=(
            jax.ShapeDtypeStruct(brick, jnp.float32),
            jax.ShapeDtypeStruct((channels, slots), jnp.float32),
        ),
        in_specs=[hbm, hbm, hbm, smem, vmem, smem, vmem],
        out_specs=(vmem, vmem),
        scratch_shapes=[
            pltpu.VMEM(brick, jnp.float32),
            pltpu.VMEM(brick, jnp.float32),
            pltpu.VMEM(brick[1:], jnp.int32),
            pltpu.VMEM(brick[1:], jnp.float32),
            pltpu.VMEM((STEPS - 1,) + brick, jnp.float32),
            pltpu.VMEM(brick, jnp.float32),
            pltpu.VMEM((STEPS, 2, channels, size_y, size_z), jnp.bfloat16),
            pltpu.VMEM((STEPS + 1, 2, channels, size_y, size_z), jnp.bfloat16),
            pltpu.VMEM((STEPS, 2, channels, size_x, size_z), jnp.float32),
            pltpu.VMEM((STEPS + 1, 2, channels, size_x, size_z), jnp.float32),
            pltpu.VMEM((STEPS, size_y, size_z), jnp.float32),
            pltpu.VMEM((STEPS + 1, 2, size_y, size_z), jnp.float32),
            pltpu.VMEM((devices, 4, slots), jnp.float32),
            pltpu.VMEM((3, slots, slots), jnp.float32),
            pltpu.VMEM((devices, slots, slots), jnp.bfloat16),
            pltpu.VMEM((ROUNDS, channels, slots), jnp.bfloat16),
            pltpu.VMEM((ROUNDS, devices, channels, slots), jnp.bfloat16),
            pltpu.SemaphoreType.DMA((3,)),
            pltpu.SemaphoreType.DMA((STEPS, 6)),
            pltpu.SemaphoreType.DMA((STEPS, 6)),
            pltpu.SemaphoreType.DMA((2,)),
            pltpu.SemaphoreType.DMA((ROUNDS, 2)),
        ],
        compiler_params=pltpu.CompilerParams(
            collective_id=0, has_side_effects=True, vmem_limit_bytes=60 * 1024 * 1024
        ),
    )(
        initial_field, source_term, cell_class, class_shift,
        surface_cell.reshape(1, slots), live_count, panel_geometry,
    )


def solution(mesh):
    placed = (
        P(None, "row", "col", "gz"),
        P(None, "row", "col", "gz"),
        P("row", "col", "gz"),
        P(),
        P(("row", "col", "gz")),
        P(("row", "col", "gz")),
        P(None, ("row", "col", "gz")),
    )
    return jax.shard_map(
        functools.partial(local, tuple(mesh.shape[axis] for axis in AXES)),
        mesh=mesh,
        in_specs=placed,
        out_specs=(P(None, "row", "col", "gz"), P(None, ("row", "col", "gz"))),
        check_vma=False,
    )
```

```python
import functools
import math

import jax
import jax.numpy as jnp
import numpy as np
from jax import lax
from jax.experimental import pallas as pl
from jax.experimental.pallas import tpu as pltpu
from jax.sharding import PartitionSpec as P

SWEEPS = 3
ROUNDS = 2
STEPS = SWEEPS * ROUNDS

relax_weight = 0.8
wave_number = 25.0
soften = 0.05
coupling = 0.5

MESH = pl.DeviceIdType.MESH
AXES = ("row", "col", "gz")


def cosine_terms(degree=8):
    nodes = 0.125 * (1.0 + np.cos(np.pi * (np.arange(64) + 0.5) / 64))
    fitted = np.polynomial.Polynomial.fit(
        nodes, np.cos(2 * np.pi * np.sqrt(nodes)), degree, domain=[0.0, 0.25]
    )
    return [float(c) for c in fitted.convert().coef]


COSINE = cosine_terms()


def cosine_of_turns(turns):
    fraction = turns - jnp.floor(turns + 0.5)
    square = fraction * fraction
    value = jnp.full_like(square, COSINE[-1])
    for term in reversed(COSINE[:-1]):
        value = value * square + term
    return value


def kernel(
    sizes,
    init_hbm, source_hbm, class_hbm, shift_hbm, cell_hbm, geo_hbm, live_ref,
    field_ref, potential_ref,
    init_v, source_v, class_v, weight_v, state_v, forcing_v,
    x_out, x_in, y_out, y_in, z_out, z_in,
    geo_all, column_v, tile_v, density_out, density_all,
    shift_ref, cell_ref, geo_ref,
    local_sem, face_send, face_recv, geo_sem, density_sem,
):
    rows, cols, depths = sizes
    devices = rows * cols * depths
    channels, size_x, size_y, size_z = init_hbm.shape
    slots = cell_hbm.shape[1]
    classes = shift_ref.shape[0]
    factor = 1.0 / math.sqrt(slots * devices)
    here = tuple(lax.axis_index(axis) for axis in AXES)
    me = (here[0] * cols + here[1]) * depths + here[2]

    copies = [
        pltpu.make_async_copy(init_hbm, init_v, local_sem.at[0]),
        pltpu.make_async_copy(class_hbm, class_v, local_sem.at[1]),
        pltpu.make_async_copy(source_hbm, source_v, local_sem.at[2]),
        pltpu.make_async_copy(geo_hbm, geo_ref, local_sem.at[3]),
        pltpu.make_async_copy(shift_hbm, shift_ref, local_sem.at[4]),
        pltpu.make_async_copy(cell_hbm, cell_ref, local_sem.at[5]),
    ]
    for copy in copies:
        copy.start()

    def each_other(action):
        def at(a, first):
            row = lax.rem(here[0] + a, rows)
            for b in range(cols):
                for c in range(depths):
                    if first and b == 0 and c == 0:
                        continue
                    action((row, lax.rem(here[1] + b, cols), lax.rem(here[2] + c, depths)))

        def others(i, carry):
            at(i, False)
            return carry

        lax.fori_loop(1, rows, others, 0)
        at(0, True)

    barrier = pltpu.get_barrier_semaphore()
    each_other(
        lambda device: pl.semaphore_signal(barrier, inc=1, device_id=device, device_id_type=MESH)
    )

    lane = lax.broadcasted_iota(jnp.int32, (size_y, size_z), 1)
    line = lax.broadcasted_iota(jnp.int32, (size_y, size_z), 0)
    pair = lane >> 1
    edge = (lane == 0) | (lane == size_z - 1)

    def pack(k, e, x, value, packed):
        if x == 0:
            x_out[k, 0, e] = value.astype(x_out.dtype)
        if x == size_x - 1:
            x_out[k, 1, e] = value.astype(x_out.dtype)
        y_out[k, 0, e, x : x + 1, :] = value[0:1, :]
        y_out[k, 1, e, x : x + 1, :] = value[size_y - 1 : size_y, :]
        at = e * size_x + x
        return jnp.where(pair == at, pltpu.roll(value, lax.rem(2 * at + 1, size_z), 1), packed)

    def face_copies(k):
        made = []
        for axis, (send, receive) in enumerate(((x_out, x_in), (y_out, y_in), (z_out, z_in))):
            count = sizes[axis]
            if count == 1:
                continue
            for up in (0, 1):
                target = {AXES[axis]: here[axis] + (1 if up else -1)}
                source = send.at[k] if axis == 2 else send.at[k, up]
                copy = pltpu.make_async_remote_copy(
                    src_ref=source,
                    dst_ref=receive.at[k, 1 - up],
                    send_sem=face_send.at[k, 2 * axis + up],
                    recv_sem=face_recv.at[k, 2 * axis + 1 - up],
                    device_id=target,
                    device_id_type=MESH,
                )
                sends = here[axis] < count - 1 if up else here[axis] > 0
                gets = here[axis] > 0 if up else here[axis] < count - 1
                made.append((copy, sends, gets))
        return made

    def start_faces(k):
        for copy, sends, _ in face_copies(k):
            pl.when(sends)(copy.start)

    def await_faces(k):
        for copy, _, gets in face_copies(k):
            pl.when(gets)(copy.wait_recv)

    def finish_faces(k):
        for copy, sends, _ in face_copies(k):
            pl.when(sends)(copy.wait_send)

    x_in[STEPS] = jnp.zeros(x_in.shape[1:], x_in.dtype)
    y_in[STEPS] = jnp.zeros(y_in.shape[1:], y_in.dtype)
    z_in[STEPS] = jnp.zeros(z_in.shape[1:], z_in.dtype)

    copies[0].wait()

    def pack_first(e, packed):
        for x in range(size_x):
            packed = pack(0, e, x, init_v[e, x], packed)
        return packed

    z_out[0] = lax.fori_loop(
        0, channels, pack_first, jnp.zeros((size_y, size_z), jnp.float32), unroll=True
    )

    copies[3].wait()
    eye = lax.broadcasted_iota(jnp.int32, (slots, slots), 0) == lax.broadcasted_iota(
        jnp.int32, (slots, slots), 1
    )
    for i in range(3):
        column = jnp.sum(jnp.where(eye, geo_ref[i : i + 1, :], 0.0), axis=1, keepdims=True)
        column_v[i] = jnp.broadcast_to(column, (slots, slots))
    geo_all[me] = geo_ref[...]

    pl.semaphore_wait(barrier, devices - 1)
    start_faces(0)

    def gather_copy(source, gathered, sems, device):
        return pltpu.make_async_remote_copy(
            src_ref=source,
            dst_ref=gathered.at[me],
            send_sem=sems.at[0],
            recv_sem=sems.at[1],
            device_id=device,
            device_id_type=MESH,
        )

    def start_gather(source, gathered, sems):
        each_other(lambda device: gather_copy(source, gathered, sems, device).start())

    def await_gather(gathered, sems, which):
        whole = gathered.at[pl.ds(0, devices - 1)]
        pltpu.make_async_copy(whole, whole, sems.at[which]).wait()

    start_gather(geo_ref, geo_all, geo_sem)

    copies[1].wait()
    copies[4].wait()
    for x in range(size_x):
        kind = class_v[x]
        shift = jnp.zeros(kind.shape, jnp.float32)
        for level in range(classes):
            shift = jnp.where(kind == level, shift_ref[level], shift)
        weight_v[x] = relax_weight / (6.0 + shift)

    copies[5].wait()
    cell = cell_ref[...]
    bits = size_z.bit_length() - 1
    cell_z = cell & (size_z - 1)
    cell_xy = cell >> bits
    pick_z = lax.broadcasted_iota(jnp.int32, (size_z, slots), 0) == cell_z
    pick_z = jnp.where(pick_z, 1.0, 0.0).astype(jnp.bfloat16)
    pick_xy = lax.broadcasted_iota(jnp.int32, (size_x * size_y, slots), 0) == cell_xy
    live = lax.broadcasted_iota(jnp.int32, (channels, slots), 1) < live_ref[0]
    which = lax.broadcasted_iota(jnp.int32, (channels, slots), 0)
    copies[2].wait()

    def now(k, e, x):
        return init_v[e, x] if k == 0 else state_v[k - 1, e, x]

    def inner(k):
        force = source_v if k <= SWEEPS else forcing_v

        def body(e, carry):
            tiles = [now(k, e, x) for x in range(size_x)]
            for x in range(size_x):
                value = tiles[x]
                around = force[e, x]
                if x + 1 < size_x:
                    around = around + tiles[x + 1]
                if x > 0:
                    around = around + tiles[x - 1]
                around = around + jnp.where(
                    line == size_y - 1, 0.0, pltpu.roll(value, size_y - 1, 0)
                )
                around = around + jnp.where(line == 0, 0.0, pltpu.roll(value, 1, 0))
                around = around + jnp.where(
                    lane == size_z - 1, 0.0, pltpu.roll(value, size_z - 1, 1)
                )
                around = around + jnp.where(lane == 0, 0.0, pltpu.roll(value, 1, 1))
                state_v[k, e, x] = (1.0 - relax_weight) * value + weight_v[x] * around
            return carry

        lax.fori_loop(0, channels, body, 0, unroll=8)

    def outer(k):
        last = k == STEPS - 1
        slot = []
        for axis in range(3):
            below = jnp.where(here[axis] > 0, k, STEPS)
            above = jnp.where(here[axis] < sizes[axis] - 1, k, STEPS)
            slot.append((below, above))
        beyond = jnp.where(
            (lane & 1) == 0, z_in[slot[2][0], 0], pltpu.roll(z_in[slot[2][1], 1], size_z - 2, 1)
        )

        def body(e, packed):
            for x in range(size_x):
                low = y_in[slot[1][0], 0, e, x : x + 1, :]
                high = y_in[slot[1][1], 1, e, x : x + 1, :]
                at = e * size_x + x
                around = jnp.where(
                    edge, pltpu.roll(beyond, lax.rem(2 * size_z - 2 * at, size_z), 1), 0.0
                )
                around = around + jnp.where(
                    line == 0, low, jnp.where(line == size_y - 1, high, 0.0)
                )
                if x == 0:
                    around = around + x_in[slot[0][0], 0, e].astype(jnp.float32)
                if x == size_x - 1:
                    around = around + x_in[slot[0][1], 1, e].astype(jnp.float32)
                result = state_v[k, e, x] + weight_v[x] * around
                if last:
                    field_ref[e, x] = result
                else:
                    state_v[k, e, x] = result
                    packed = pack(k + 1, e, x, result, packed)
            return packed

        packed = lax.fori_loop(
            0, channels, body, jnp.zeros((size_y, size_z), jnp.float32), unroll=8
        )
        if not last:
            z_out[k + 1] = packed

    pieces = 4
    chunk = slots // pieces

    def make_tiles(first, stop):
        def body(s, carry):
            source = geo_all[s]
            values = []
            for piece in range(pieces):
                span = slice(piece * chunk, (piece + 1) * chunk)
                delta_x = column_v[0, span, :] - source[0:1, :]
                delta_y = column_v[1, span, :] - source[1:2, :]
                delta_z = column_v[2, span, :] - source[2:3, :]
                distance = jnp.sqrt(delta_x * delta_x + delta_y * delta_y + delta_z * delta_z)
                wave = cosine_of_turns(distance * (wave_number / (2.0 * math.pi)))
                value = (source[3:4, :] * factor) * wave / (distance + soften)
                values.append(value)
            turned = jnp.concatenate(values, axis=0).T
            tile_v[pl.ds(pl.multiple_of(s * slots, slots), slots), :] = turned.astype(tile_v.dtype)
            return carry

        lax.fori_loop(first, stop, body, 0)

    group = math.gcd(devices, 8)

    def apply_tiles(gathered):
        def body(i, total):
            values = jnp.concatenate([gathered[i * group + j] for j in range(group)], axis=1)
            span = pl.ds(pl.multiple_of(i * group * slots, group * slots), group * slots)
            return total + jnp.dot(values, tile_v[span, :], preferred_element_type=jnp.float32)

        return lax.fori_loop(
            0, devices // group, body, jnp.zeros((channels, slots), jnp.float32)
        )

    cut = [0, devices // 4, devices // 2, devices]
    for k in range(STEPS):
        if k != SWEEPS:
            inner(k)
        if k == 1:
            await_gather(geo_all, geo_sem, 1)
        if k in (1, 2):
            make_tiles(cut[k - 1], cut[k])
        await_faces(k)
        outer(k)
        end = k % SWEEPS == SWEEPS - 1
        if k + 1 < STEPS:
            start_faces(k + 1)
        if not end:
            continue
        r = k // SWEEPS
        ending = field_ref if k == STEPS - 1 else state_v.at[k]
        flat = ending[...].reshape(channels * size_x * size_y, size_z).astype(jnp.bfloat16)
        picked = jnp.dot(flat, pick_z, preferred_element_type=jnp.float32)
        density = jnp.zeros((channels, slots), jnp.float32)
        for e in range(channels):
            block = picked[e * size_x * size_y : (e + 1) * size_x * size_y]
            found = jnp.sum(jnp.where(pick_xy, block, 0.0), axis=0, keepdims=True)
            density = jnp.where(which == e, found, density)
        density = jnp.where(live, density, 0.0).astype(jnp.bfloat16)
        density_out[r] = density
        density_all[r, me] = density
        start_gather(density_out.at[r], density_all.at[r], density_sem.at[r])
        if r < ROUNDS - 1:
            inner(k + 1)
        if r == 0:
            make_tiles(cut[2], cut[3])
        await_gather(density_all.at[r], density_sem.at[r], 1)
        potential = jnp.where(live, apply_tiles(density_all.at[r]), 0.0)
        if r == ROUNDS - 1:
            potential_ref[...] = potential
        else:
            half_of = coupling * potential
            big = half_of.astype(jnp.bfloat16).astype(jnp.float32)
            small = half_of - big
            for e in range(channels):
                load = jnp.zeros((size_x * size_y, size_z), jnp.float32)
                for part in (big, small):
                    placed = jnp.where(pick_xy, part[e : e + 1, :], 0.0).astype(jnp.bfloat16)
                    load = load + lax.dot_general(
                        placed, pick_z, (((1,), (1,)), ((), ())),
                        preferred_element_type=jnp.float32,
                    )
                load = load.reshape(size_x, size_y, size_z)
                forcing_v[e] = source_v[e] + load
                state_v[k + 1, e] = state_v[k + 1, e] + weight_v[...] * load

    for k in range(STEPS):
        finish_faces(k)
    await_gather(geo_all, geo_sem, 0)
    for r in range(ROUNDS):
        await_gather(density_all.at[r], density_sem.at[r], 0)


def local(sizes, initial_field, source_term, cell_class, class_shift, surface_cell, live_count,
          panel_geometry):
    channels, size_x, size_y, size_z = initial_field.shape
    slots = surface_cell.shape[0]
    devices = sizes[0] * sizes[1] * sizes[2]
    brick = (channels, size_x, size_y, size_z)
    vmem = pl.BlockSpec(memory_space=pltpu.VMEM)
    hbm = pl.BlockSpec(memory_space=pltpu.HBM)
    per_device = slots * (2 * slots + 4 * 8 + ROUNDS * 2 * channels)
    grant = devices * per_device + 24 * 4 * math.prod(brick)
    operands = [
        pltpu.with_memory_space_constraint(array, pltpu.HBM)
        for array in (
            initial_field, source_term, cell_class, class_shift,
            surface_cell.reshape(1, slots), panel_geometry,
        )
    ]
    operands.append(live_count)
    return pl.pallas_call(
        functools.partial(kernel, sizes),
        out_shape=(
            jax.ShapeDtypeStruct(brick, jnp.float32),
            jax.ShapeDtypeStruct((channels, slots), jnp.float32),
        ),
        in_specs=[hbm] * 6 + [pl.BlockSpec(memory_space=pltpu.SMEM)],
        out_specs=(vmem, vmem),
        scratch_shapes=[
            pltpu.VMEM(brick, jnp.float32),
            pltpu.VMEM(brick, jnp.float32),
            pltpu.VMEM(brick[1:], jnp.int32),
            pltpu.VMEM(brick[1:], jnp.float32),
            pltpu.VMEM((STEPS,) + brick, jnp.float32),
            pltpu.VMEM(brick, jnp.float32),
            pltpu.VMEM((STEPS, 2, channels, size_y, size_z), jnp.bfloat16),
            pltpu.VMEM((STEPS + 1, 2, channels, size_y, size_z), jnp.bfloat16),
            pltpu.VMEM((STEPS, 2, channels, size_x, size_z), jnp.float32),
            pltpu.VMEM((STEPS + 1, 2, channels, size_x, size_z), jnp.float32),
            pltpu.VMEM((STEPS, size_y, size_z), jnp.float32),
            pltpu.VMEM((STEPS + 1, 2, size_y, size_z), jnp.float32),
            pltpu.VMEM((devices, 4, slots), jnp.float32),
            pltpu.VMEM((3, slots, slots), jnp.float32),
            pltpu.VMEM((devices * slots, slots), jnp.bfloat16),
            pltpu.VMEM((ROUNDS, channels, slots), jnp.bfloat16),
            pltpu.VMEM((ROUNDS, devices, channels, slots), jnp.bfloat16),
            pltpu.SMEM(class_shift.shape, jnp.float32),
            pltpu.VMEM((1, slots), jnp.int32),
            pltpu.VMEM(panel_geometry.shape, jnp.float32),
            pltpu.SemaphoreType.DMA((6,)),
            pltpu.SemaphoreType.DMA((STEPS, 6)),
            pltpu.SemaphoreType.DMA((STEPS, 6)),
            pltpu.SemaphoreType.DMA((2,)),
            pltpu.SemaphoreType.DMA((ROUNDS, 2)),
        ],
        compiler_params=pltpu.CompilerParams(
            collective_id=0, has_side_effects=True, vmem_limit_bytes=grant
        ),
    )(*operands)


def solution(mesh):
    placed = (
        P(None, "row", "col", "gz"),
        P(None, "row", "col", "gz"),
        P("row", "col", "gz"),
        P(),
        P(("row", "col", "gz")),
        P(("row", "col", "gz")),
        P(None, ("row", "col", "gz")),
    )
    return jax.shard_map(
        functools.partial(local, tuple(mesh.shape[axis] for axis in AXES)),
        mesh=mesh,
        in_specs=placed,
        out_specs=(P(None, "row", "col", "gz"), P(None, ("row", "col", "gz"))),
        check_vma=False,
    )
```
